32 devices in a mesh: replica: 2 (over x), tp: 16 (over z, y, core).
Axes of the slice: x: 2, y: 2, z: 4, core: 2. Of those that a mesh axis runs over, the one named last changes fastest.
Arguments:
- hidden_in: bfloat16 [8, 16384], P('replica', 'tp'), parts along dimension 0, may hold values from -60 to 60
- norm_gain: bfloat16 [16384], P('tp'), may hold values from 0.5 to 1.5
- w_qkv: bfloat16 [16384, 9216], P(None, 'tp'), may hold values from -0.046875 to 0.046875
- w_out: bfloat16 [8192, 16384], P('tp'), may hold values from -0.09375 to 0.09375
- key_cache: bfloat16 [8, 2048, 512], P('replica', 'tp'), parts along dimension 0, may hold values from -1200 to 1200
- value_cache: bfloat16 [8, 2048, 512], P('replica', 'tp'), parts along dimension 0, may hold values from -6 to 6
- lengths: int32 [8], P('replica'), parts along dimension 0, may hold values from 1024 to 2048
- positions: int32 [8], P('replica'), parts along dimension 0, may hold values from 0 to 4095
Outputs:
- attn_out: bfloat16 [8, 16384], P('replica', 'tp'), parts along dimension 0
- token_scale: float32 [8], P('replica'), parts along dimension 0
The draws below stay inside these ranges and needn't reach their ends.
There are 2 independent parts, one for each index of `replica`. The reference program is written for one: setup_inputs(seed, part) draws one part's arguments, and reference() takes and returns one part's arrays. A program takes and returns all parts, laid end to end along the dimension named above; an argument that names none is the same for every part. Nothing has to cross between parts.
All inputs are finite; a program needn't handle non-finite values.
Results may differ from the reference program's by a relative error of at most 0.017.
The reference program's roundings to bfloat16 on the way count: a program that leaves them out, or rounds other values in their place, can miss the bound.
Values may be sent and summed in bfloat16 or wider, within the bound.
A program may use at most 128 MiB of HBM per device.

```python
import jax
import jax.numpy as jnp
from jax import lax

D = 16384
QUERY_HEADS = 64
KEY_VALUE_HEADS = 4
HEAD_SIZE = 128
BATCH_SEQUENCES = 4
DEVICE_POSITIONS = 128
CACHE_POSITIONS = 2048
QKVW = 9216


def draw_hidden_in(key, part):
    leading_part, second = jax.random.split(key, 2)
    column = jnp.exp(jax.random.uniform(second, (D,), jnp.float32, 0.0, jnp.log(10.0)))
    values = jnp.clip(jax.random.normal(leading_part, (BATCH_SEQUENCES, D), jnp.float32), -6.0, 6.0) * column[None, :]
    return jnp.clip(values, -60.0, 60.0).astype(jnp.bfloat16)


def draw_key_cache(key, part):
    leading_part = jax.random.fold_in(key, 0)
    offset_start = jnp.clip(jax.random.normal(leading_part, (BATCH_SEQUENCES, CACHE_POSITIONS, KEY_VALUE_HEADS * HEAD_SIZE), jnp.float32), -6.0, 6.0)
    return jnp.clip(offset_start, -1200.0, 1200.0).astype(jnp.bfloat16)


def touch_ends(entries, rng, smallest, high):
    index_at = [jax.random.randint(jax.random.fold_in(rng, axis), (), 0, length) for axis, length in enumerate(entries.shape)]
    longest = entries.shape.index(max(entries.shape))
    next_to = index_at[:longest] + [(index_at[longest] + 1) % entries.shape[longest]] + index_at[longest + 1:]
    return entries.at[tuple(index_at)].set(smallest).at[tuple(next_to)].set(high)


def raised(result, key, source, target, blocks, factor):
    owner, partner = [(jnp.arange(result.shape[axis_at]) // (result.shape[axis_at] // blocks)).reshape([-1 if axis == axis_at else 1 for axis in range(result.ndim)]) for axis_at in (source, target)]
    chosen = jax.random.permutation(key, blocks)[partner]
    strong = (owner == chosen) | (owner == (partner + blocks // 2) % blocks)
    return jnp.where(strong, factor * result, result)


def levels(own_key, dims, pieces, smallest, high):
    factor_of, own = 1.0, jax.random.fold_in(own_key, 6)
    for dim, shards_of in pieces:
        steps = jnp.exp(jax.random.uniform(jax.random.fold_in(own, dim), (shards_of,), jnp.float32, smallest / len(pieces), high / len(pieces)))
        factor_of = factor_of * jnp.repeat(steps, dims[dim] // shards_of).reshape([-1 if axis == dim else 1 for axis in range(len(dims))])
    return factor_of


def gaussian(rng, shape, scale, limit, pieces=(), kind=jnp.bfloat16):
    gain = levels(rng, shape, pieces, -0.22, 0.18) if pieces else 1.0
    values = jax.random.normal(rng, shape, jnp.float32) * scale * gain
    return jnp.minimum(jnp.maximum(values, -limit), limit).astype(kind)


def gaussian_with(own_key, shape, scale, bound, cuts, heavy, kind=jnp.bfloat16):
    drawn = scale * jax.random.normal(own_key, shape, jnp.float32)
    if cuts:
        drawn = drawn * levels(own_key, shape, cuts, -0.22, 0.18)
    return jnp.clip(raised(drawn, jax.random.fold_in(own_key, 3), *heavy), -bound, bound).astype(kind)


def setup_inputs(seed: int = 0, part: int = 0) -> dict:
    keys = jax.random.split(jax.random.key(seed), 9)
    own_keys = jax.random.split(jax.random.fold_in(keys[8], part), 9)
    hidden_in = draw_hidden_in(jax.random.fold_in(jax.random.fold_in(keys[8], part), 71), part)
    norm_gain = jnp.clip(1.0 + 0.1 * jax.random.normal(keys[1], (D,), jnp.float32), 0.5, 1.5).astype(jnp.bfloat16)
    w_qkv = gaussian(keys[2], (D, QKVW), D ** -0.5, 0.046875, ((1, 16),))
    w_out = gaussian_with(keys[3], (QUERY_HEADS * HEAD_SIZE, D), (QUERY_HEADS * HEAD_SIZE) ** -0.5, 0.09375, ((0, 16),), (0, 1, 16, 2.0))
    key_cache = draw_key_cache(jax.random.fold_in(jax.random.fold_in(keys[8], part), 71), part)
    value_cache = gaussian(own_keys[5], (BATCH_SEQUENCES, CACHE_POSITIONS, KEY_VALUE_HEADS * HEAD_SIZE), 1.0, 6.0, ((1, 16),))
    lengths = touch_ends(jax.random.randint(own_keys[6], (BATCH_SEQUENCES,), CACHE_POSITIONS // 2, CACHE_POSITIONS + 1), jax.random.fold_in(own_keys[6], 1), CACHE_POSITIONS // 2, CACHE_POSITIONS).astype(jnp.int32)
    positions = touch_ends(jax.random.randint(own_keys[7], (BATCH_SEQUENCES,), 0, 2 * CACHE_POSITIONS), jax.random.fold_in(own_keys[7], 1), 0, (2 * CACHE_POSITIONS) - 1).astype(jnp.int32)
    return dict(hidden_in=hidden_in, norm_gain=norm_gain, w_qkv=w_qkv, w_out=w_out, key_cache=key_cache, value_cache=value_cache, lengths=lengths, positions=positions)


def apply_rotation(heads, positions):
    half = HEAD_SIZE // 2
    freq = 500000.0 ** (-(jnp.arange(half, dtype=jnp.float32) * 2.0) / HEAD_SIZE)
    angle = positions.astype(jnp.float32)[:, None] * freq[None, :]
    cosine = jnp.cos(angle)[:, None, :]
    sine = jnp.sin(angle)[:, None, :]
    leading_part = heads[..., :half]
    second = heads[..., half:]
    return jnp.concatenate([leading_part * cosine - second * sine, second * cosine + leading_part * sine], axis=-1)

def reference(hidden_in, norm_gain, w_qkv, w_out, key_cache, value_cache, lengths, positions):
    batch_count = hidden_in.shape[0]
    group_count = QUERY_HEADS // KEY_VALUE_HEADS
    block_list = CACHE_POSITIONS // DEVICE_POSITIONS
    query_width = QUERY_HEADS * HEAD_SIZE
    key_width = KEY_VALUE_HEADS * HEAD_SIZE
    inv = 1.0 / HEAD_SIZE ** 0.5
    values = hidden_in.astype(jnp.float32)
    rstd = lax.rsqrt(lax.optimization_barrier(jnp.mean(values * values, axis=-1)) + 1e-05)
    normed = values * norm_gain.astype(jnp.float32)[None, :] * rstd[:, None]
    token_scale = (lax.optimization_barrier(jnp.max(jnp.abs(normed), axis=-1)) + 1e-06) / 448.0
    quant = (normed / token_scale[:, None]).astype(jnp.bfloat16)
    query_key_value = (jnp.dot(quant, w_qkv, preferred_element_type=jnp.float32) * token_scale[:, None]).astype(jnp.bfloat16)
    query_rows = apply_rotation(query_key_value[:, :query_width].astype(jnp.float32).reshape(batch_count, QUERY_HEADS, HEAD_SIZE), positions).astype(jnp.bfloat16)
    latest_key = apply_rotation(query_key_value[:, query_width:query_width + key_width].astype(jnp.float32).reshape(batch_count, KEY_VALUE_HEADS, HEAD_SIZE), positions)
    latest_value = query_key_value[:, query_width + key_width:].astype(jnp.float32).reshape(batch_count, KEY_VALUE_HEADS, HEAD_SIZE)
    grouped_query = query_rows.astype(jnp.float32).reshape(batch_count, KEY_VALUE_HEADS, group_count, HEAD_SIZE)
    key_rows = key_cache.astype(jnp.float32).reshape(batch_count, block_list, DEVICE_POSITIONS, KEY_VALUE_HEADS, HEAD_SIZE)
    value_rows = value_cache.astype(jnp.float32).reshape(batch_count, block_list, DEVICE_POSITIONS, KEY_VALUE_HEADS, HEAD_SIZE)
    scores = jnp.einsum('bgjd,bnpgd->bgjnp', grouped_query, key_rows) * inv
    where_pos = jnp.arange(CACHE_POSITIONS, dtype=jnp.int32).reshape(block_list, DEVICE_POSITIONS)
    valid = (where_pos[None, :, :] < lengths[:, None, None])[:, None, None, :, :]
    block_max = lax.optimization_barrier(jnp.max(jnp.where(valid, scores, -1e+30), axis=-1))
    weights = jnp.where(valid, jnp.exp(scores - block_max[..., None]), 0.0)
    block_sum = lax.optimization_barrier(jnp.sum(weights, axis=-1))
    rounded = lax.optimization_barrier(weights.astype(jnp.bfloat16)).astype(jnp.float32)
    block_out = jnp.einsum('bgjnp,bnpgd->bgjnd', rounded, value_rows)
    top = lax.optimization_barrier(jnp.max(block_max, axis=-1))
    factor = jnp.exp(block_max - top[..., None])
    total = lax.optimization_barrier(jnp.sum(block_sum * factor, axis=-1))
    summed = lax.optimization_barrier(jnp.sum(block_out * factor[..., None], axis=-2))
    score_new = jnp.einsum('bgjd,bgd->bgj', grouped_query, latest_key) * inv
    top_new = jnp.maximum(top, score_new)
    keep = jnp.exp(top - top_new)
    fresh = jnp.exp(score_new - top_new)
    total = total * keep + fresh
    summed = summed * keep[..., None] + fresh[..., None] * latest_value[:, :, None, :]
    att = (summed / total[..., None]).reshape(batch_count, query_width).astype(jnp.bfloat16)
    attn_out = jnp.dot(att, w_out, preferred_element_type=jnp.float32).astype(jnp.bfloat16)
    return (attn_out, token_scale)
```

```python
import functools

import jax
import jax.numpy as jnp
import numpy as np
from jax import lax
from jax.experimental import pallas as pl
from jax.experimental.pallas import tpu as pltpu
from jax.sharding import PartitionSpec as P

QUERY_HEADS = 64
KEY_VALUE_HEADS = 4
HEAD_SIZE = 128
LANES = 128


def rounded_up(value, step):
    return (value + step - 1) // step * step


def kernel(
    n,
    hidden_hbm,
    gain_hbm,
    wq_hbm,
    wo_hbm,
    key_hbm,
    value_hbm,
    lens_ref,
    pos_ref,
    freq_ref,
    out_ref,
    scale_ref,
    xg,
    gg,
    gained,
    quant,
    wq,
    wo,
    kv,
    vv,
    qg,
    heads,
    so,
    og,
    rs_send,
    rs_recv,
    x_local,
    g_local,
    wq_sem,
    wo_sem,
    kv_sem,
    x_send,
    x_recv,
    g_send,
    g_recv,
    q_send,
    q_recv,
    o_send,
    o_recv,
    r_send,
    r_recv,
):
    me = lax.axis_index("tp")
    batch, dx = hidden_hbm.shape
    width = wq_hbm.shape[0]
    cw = wq_hbm.shape[1]
    padded = qg.shape[2]
    own_rows = og.shape[1]
    own_heads = own_rows // batch
    positions = key_hbm.shape[1]
    group = QUERY_HEADS // KEY_VALUE_HEADS
    f32, bf16 = jnp.float32, jnp.bfloat16

    def wq_copy(c):
        return pltpu.make_async_copy(
            wq_hbm.at[pl.ds(pl.multiple_of(c * dx, dx), dx), :], wq.at[c], wq_sem.at[c]
        )

    def wo_copy(c):
        return pltpu.make_async_copy(
            wo_hbm.at[:, pl.ds(pl.multiple_of(c * dx, dx), dx)], wo.at[c], wo_sem.at[c]
        )

    def remote(src, dst, send, recv, peer):
        return pltpu.make_async_remote_copy(
            src_ref=src,
            dst_ref=dst,
            send_sem=send,
            recv_sem=recv,
            device_id={"tp": peer},
            device_id_type=pl.DeviceIdType.MESH,
        )

    def each_peer(act):
        def step(k, carry):
            act(lax.rem(me + k, n))
            return carry

        lax.fori_loop(1, n, step, 0)

    local_x = pltpu.make_async_copy(hidden_hbm, xg.at[me], x_local)
    local_g = pltpu.make_async_copy(gain_hbm, gg.at[me], g_local)
    local_x.start()
    local_g.start()

    barrier = pltpu.get_barrier_semaphore()
    each_peer(
        lambda peer: pl.semaphore_signal(
            barrier, inc=1, device_id={"tp": peer}, device_id_type=pl.DeviceIdType.MESH
        )
    )

    def start_wq(c, carry):
        wq_copy(c).start()
        return carry

    lax.fori_loop(0, n, start_wq, 0)
    copy_k = pltpu.make_async_copy(key_hbm, kv, kv_sem.at[0])
    copy_v = pltpu.make_async_copy(value_hbm, vv, kv_sem.at[1])
    copy_k.start()
    copy_v.start()

    def start_wo(k, carry):
        wo_copy(lax.rem(me + 1 + k, n)).start()
        return carry

    lax.fori_loop(0, n, start_wo, 0)

    row4 = lax.broadcasted_iota(jnp.int32, (8, LANES), 0) % batch
    place = jnp.zeros((8, LANES), f32)
    for b in range(batch):
        place = jnp.where(row4 == b, pos_ref[b].astype(f32), place)
    angle = place * freq_ref[...]
    cosine = jnp.cos(angle)
    sine = jnp.sin(angle)
    lane8 = lax.broadcasted_iota(jnp.int32, (8, LANES), 1)
    sine = jnp.where(lane8 < HEAD_SIZE // 2, -sine, sine)

    local_x.wait()
    local_g.wait()
    pl.semaphore_wait(barrier, n - 1)

    def send_x(peer):
        remote(xg.at[me], xg.at[me], x_send.at[peer], x_recv.at[me], peer).start()
        remote(gg.at[me], gg.at[me], g_send.at[peer], g_recv.at[me], peer).start()

    each_peer(send_x)

    def gain_piece(s, squares, peak):
        for j in range(dx // LANES):
            x = xg[s, :, j * LANES : (j + 1) * LANES].astype(f32)
            g = gg[s, j : j + 1, :].astype(f32)
            squares = squares + x * x
            y = x * g
            gained[s, :, j * LANES : (j + 1) * LANES] = y
            peak = jnp.maximum(peak, jnp.abs(y))
        return squares, peak

    zero = jnp.zeros((batch, LANES), f32)
    squares, peak = gain_piece(me, zero, zero)

    def take_x(k, carry):
        s = lax.rem(me + k, n)
        remote(xg.at[s], xg.at[s], x_send.at[s], x_recv.at[s], s).wait_recv()
        remote(gg.at[s], gg.at[s], g_send.at[s], g_recv.at[s], s).wait_recv()
        return gain_piece(s, *carry)

    squares, peak = lax.fori_loop(1, n, take_x, (squares, peak))
    rstd = lax.rsqrt(jnp.sum(squares, axis=-1, keepdims=True) / width + 1e-05)
    token_scale = (jnp.max(peak, axis=-1, keepdims=True) * rstd + 1e-06) / 448.0
    for b in range(batch):
        scale_ref[b] = jnp.max(token_scale[b : b + 1, :])

    per = 4 if n % 4 == 0 else 1

    def project(i, acc):
        for u in range(per):
            c = i * per + u
            wq_copy(c).wait()
            quant[c] = (gained[c] * rstd / token_scale).astype(bf16)
        for u in range(per):
            c = i * per + u
            acc = acc + jnp.dot(quant[c], wq[c], preferred_element_type=f32)
        return acc

    acc = lax.fori_loop(0, n // per, project, jnp.zeros((batch, cw), f32))
    proj = (acc * token_scale).astype(bf16).astype(f32)
    if padded > cw:
        proj = jnp.concatenate([proj, jnp.zeros((batch, padded - cw), f32)], axis=1)
    if cw % LANES:
        proj = pltpu.roll(proj, lax.rem(me * cw, LANES), 1)
    qg[me] = proj.astype(bf16)
    each_peer(
        lambda peer: remote(
            qg.at[me], qg.at[me], q_send.at[peer], q_recv.at[me], peer
        ).start()
    )
    each_peer(lambda s: remote(qg.at[s], qg.at[s], q_send.at[s], q_recv.at[s], s).wait_recv())

    total_heads = QUERY_HEADS + 2 * KEY_VALUE_HEADS
    for h in range(total_heads):
        piece = None
        for d in range(h * LANES // cw, (h * LANES + LANES - 1) // cw + 1):
            block = h - d * cw // LANES
            part = qg[d, :, block * LANES : (block + 1) * LANES].astype(f32)
            piece = part if piece is None else piece + part
        heads[h * batch : (h + 1) * batch, :] = piece

    def rotated(rows):
        count = rows.shape[0]
        turned = pltpu.roll(rows, HEAD_SIZE // 2, 1)
        return rows * jnp.tile(cosine, (count // 8, 1)) + turned * jnp.tile(sine, (count // 8, 1))

    copy_k.wait()
    copy_v.wait()
    inv = 1.0 / HEAD_SIZE**0.5
    rows_g = group * batch
    cols = batch * positions
    col = lax.broadcasted_iota(jnp.int32, (8, cols), 1)
    row = lax.broadcasted_iota(jnp.int32, (8, cols), 0)
    limit = jnp.zeros((8, cols), jnp.int32)
    for b in range(batch):
        limit = jnp.where(col // positions == b, lens_ref[b], limit)
    valid8 = (row % batch == col // positions) & (me * positions + col % positions < limit)
    bias8 = jnp.where(valid8, 0.0, -1e30)
    bias = jnp.tile(bias8, (rows_g // 8, 1))
    valid = bias == 0.0
    fresh_rows = rotated(
        heads[QUERY_HEADS * batch : (QUERY_HEADS + KEY_VALUE_HEADS) * batch, :]
    )
    lane = lax.broadcasted_iota(jnp.int32, (rows_g, LANES), 1)
    for g in range(KEY_VALUE_HEADS):
        q = rotated(heads[g * rows_g : (g + 1) * rows_g, :]).astype(bf16)
        k_rows = kv[:, :, g * HEAD_SIZE : (g + 1) * HEAD_SIZE].reshape(cols, HEAD_SIZE)
        v_rows = vv[:, :, g * HEAD_SIZE : (g + 1) * HEAD_SIZE].reshape(cols, HEAD_SIZE)
        s = (
            lax.dot_general(q, k_rows, (((1,), (1,)), ((), ())), preferred_element_type=f32) * inv
        )
        top = jnp.max(jnp.where(valid, s, -1e30), axis=-1, keepdims=True)
        w = jnp.where(valid, jnp.exp(s - top), 0.0)
        total = jnp.sum(w, axis=-1, keepdims=True)
        o = jnp.dot(w.astype(bf16), v_rows, preferred_element_type=f32)
        k_new = fresh_rows[g * batch : (g + 1) * batch, :]
        base = (QUERY_HEADS + KEY_VALUE_HEADS + g) * batch
        v_new = heads[base : base + batch, :]
        s_new = (
            jnp.sum(q.astype(f32) * jnp.tile(k_new, (group, 1)), axis=-1, keepdims=True) * inv
        )
        s_new = jnp.where(me == 0, s_new, -1e30)
        top_new = jnp.maximum(top, s_new)
        keep = jnp.exp(top - top_new)
        fresh = jnp.where(me == 0, jnp.exp(s_new - top_new), 0.0)
        total = total * keep + fresh
        o = o * keep + fresh * jnp.tile(v_new, (group, 1))
        some = total > 0.0
        safe = jnp.where(some, total, 1.0)
        o = o / safe
        lse = jnp.where(some, top_new + jnp.log(safe), -1e30)
        hi = lse.astype(bf16).astype(f32)
        rest = lse - hi
        mid = rest.astype(bf16).astype(f32)
        low = rest - mid
        tail = jnp.where(
            lane == 0, hi, jnp.where(lane == 1, mid, jnp.where(lane == 2, low, 0.0))
        )
        both = jnp.concatenate([o, tail], axis=1).astype(bf16)
        for j in range(group // own_heads):
            so[g * (group // own_heads) + j] = both[j * own_rows : (j + 1) * own_rows, :]

    each_peer(
        lambda peer: remote(
            so.at[peer], og.at[me], o_send.at[peer], o_recv.at[me], peer
        ).start()
    )
    og[me] = so[me]
    each_peer(lambda s: remote(so.at[s], og.at[s], o_send.at[s], o_recv.at[s], s).wait_recv())

    lses = [
        jnp.sum(og[s, :, LANES : 2 * LANES].astype(f32), axis=-1, keepdims=True) for s in range(n)
    ]
    best = functools.reduce(jnp.maximum, lses)
    den = jnp.zeros_like(best)
    num = jnp.zeros((own_rows, LANES), f32)
    for s in range(n):
        share = jnp.exp(lses[s] - best)
        den = den + share
        num = num + share * og[s, :, 0:LANES].astype(f32)
    att = num / den
    att = jnp.concatenate(
        [att[j * batch : (j + 1) * batch, :] for j in range(own_heads)], axis=1
    ).astype(bf16)

    def project_out(k, carry):
        e = lax.rem(me + 1 + k, n)
        wo_copy(e).wait()
        rs_send[e] = jnp.dot(att, wo[e], preferred_element_type=f32).astype(bf16)
        remote(rs_send.at[e], rs_recv.at[me], r_send.at[e], r_recv.at[me], e).start()
        return carry

    lax.fori_loop(0, n - 1, project_out, 0)
    wo_copy(me).wait()
    own = jnp.dot(att, wo[me], preferred_element_type=f32)

    def take_r(k, carry):
        s = lax.rem(me + k, n)
        remote(rs_send.at[s], rs_recv.at[s], r_send.at[s], r_recv.at[s], s).wait_recv()
        return carry + rs_recv[s].astype(f32)

    out_ref[...] = lax.fori_loop(1, n, take_r, own).astype(bf16)

    def finish(peer):
        remote(xg.at[me], xg.at[me], x_send.at[peer], x_recv.at[me], peer).wait_send()
        remote(gg.at[me], gg.at[me], g_send.at[peer], g_recv.at[me], peer).wait_send()
        remote(qg.at[me], qg.at[me], q_send.at[peer], q_recv.at[me], peer).wait_send()
        remote(so.at[peer], og.at[me], o_send.at[peer], o_recv.at[me], peer).wait_send()
        remote(rs_send.at[peer], rs_recv.at[me], r_send.at[peer], r_recv.at[me], peer).wait_send()

    each_peer(finish)


def on_device(n, hidden_in, norm_gain, w_qkv, w_out, key_cache, value_cache, lengths, positions):
    batch, dx = hidden_in.shape
    width, cw = w_qkv.shape
    own_rows = w_out.shape[0] // HEAD_SIZE * batch
    total_heads = QUERY_HEADS + 2 * KEY_VALUE_HEADS
    widest = max(d * cw % LANES for d in range(n)) + cw
    padded = rounded_up(widest, LANES)
    half = HEAD_SIZE // 2
    freq = np.float32(500000.0) ** (
        -(np.arange(half, dtype=np.float32) * np.float32(2.0)) / np.float32(HEAD_SIZE)
    )
    freq = jnp.asarray(np.tile(freq.astype(np.float32), 2)[None, :])
    bf16, f32 = jnp.bfloat16, jnp.float32
    dma = pltpu.SemaphoreType.DMA
    hbm = pl.BlockSpec(memory_space=pl.ANY)
    smem = pl.BlockSpec(memory_space=pltpu.SMEM)
    vmem = pl.BlockSpec(memory_space=pltpu.VMEM)
    return pl.pallas_call(
        functools.partial(kernel, n),
        out_shape=(
            jax.ShapeDtypeStruct((batch, dx), bf16),
            jax.ShapeDtypeStruct((batch,), f32),
        ),
        in_specs=[hbm] * 6 + [smem, smem, vmem],
        out_specs=(vmem, smem),
        scratch_shapes=[
            pltpu.VMEM((n, batch, dx), bf16),
            pltpu.VMEM((n, dx // LANES, LANES), bf16),
            pltpu.VMEM((n, batch, dx), f32),
            pltpu.VMEM((n, batch, dx), bf16),
            pltpu.VMEM((n, dx, cw), bf16),
            pltpu.VMEM((n, w_out.shape[0], dx), bf16),
            pltpu.VMEM(key_cache.shape, bf16),
            pltpu.VMEM(value_cache.shape, bf16),
            pltpu.VMEM((n, batch, padded), bf16),
            pltpu.VMEM((total_heads * batch, HEAD_SIZE), f32),
            pltpu.VMEM((n, own_rows, 2 * LANES), bf16),
            pltpu.VMEM((n, own_rows, 2 * LANES), bf16),
            pltpu.VMEM((n, batch, dx), bf16),
            pltpu.VMEM((n, batch, dx), bf16),
            dma(()),
            dma(()),
            dma((n,)),
            dma((n,)),
            dma((2,)),
        ]
        + [dma((n,))] * 10,
        compiler_params=pltpu.CompilerParams(
            collective_id=0, has_side_effects=True, vmem_limit_bytes=60 * 1024 * 1024
        ),
        name="decode",
    )(
        hidden_in,
        norm_gain.reshape(dx // LANES, LANES),
        w_qkv,
        w_out,
        key_cache,
        value_cache,
        lengths,
        positions,
        freq,
    )


def solution(mesh):
    placed = (
        P("replica", "tp"),
        P("tp"),
        P(None, "tp"),
        P("tp", None),
        P("replica", "tp", None),
        P("replica", "tp", None),
        P("replica"),
        P("replica"),
    )
    return jax.shard_map(
        functools.partial(on_device, mesh.shape["tp"]),
        mesh=mesh,
        in_specs=placed,
        out_specs=(P("replica", "tp"), P("replica")),
        check_vma=False,
    )
```

```python
import functools

import jax
import jax.numpy as jnp
import numpy as np
from jax import lax
from jax.experimental import pallas as pl
from jax.experimental.pallas import tpu as pltpu
from jax.sharding import PartitionSpec as P

QUERY_HEADS = 64
KEY_VALUE_HEADS = 4
HEAD_SIZE = 128
LANES = 128


def rounded_up(value, step):
    return (value + step - 1) // step * step


def kernel(
    n,
    hidden_hbm,
    gain_hbm,
    wq_hbm,
    wo_hbm,
    key_hbm,
    value_hbm,
    lens_ref,
    pos_ref,
    freq_ref,
    out_ref,
    scale_ref,
    xg,
    gg,
    gained,
    quant,
    wq,
    wo,
    kv,
    vv,
    qg,
    heads,
    so,
    og,
    rs_send,
    rs_recv,
    x_local,
    g_local,
    wq_sem,
    wo_sem,
    kv_sem,
    x_send,
    x_recv,
    g_send,
    g_recv,
    q_send,
    q_recv,
    o_send,
    o_recv,
    r_send,
    r_recv,
):
    me = lax.axis_index("tp")
    batch, dx = hidden_hbm.shape
    cw, width = wq_hbm.shape
    padded = qg.shape[2]
    own_rows = og.shape[1]
    own_heads = own_rows // batch
    positions = key_hbm.shape[1]
    group = QUERY_HEADS // KEY_VALUE_HEADS
    f32, bf16 = jnp.float32, jnp.bfloat16

    def wq_copy(c):
        span = pl.ds(pl.multiple_of(c * dx, dx), dx)
        return pltpu.make_async_copy(wq_hbm.at[:, span], wq.at[:, span], wq_sem.at[c])

    def wo_copy(c):
        return pltpu.make_async_copy(
            wo_hbm.at[:, pl.ds(pl.multiple_of(c * dx, dx), dx)], wo.at[c], wo_sem.at[c]
        )

    def remote(src, dst, send, recv, peer):
        return pltpu.make_async_remote_copy(
            src_ref=src,
            dst_ref=dst,
            send_sem=send,
            recv_sem=recv,
            device_id={"tp": peer},
            device_id_type=pl.DeviceIdType.MESH,
        )

    def each_peer(act):
        def step(k, carry):
            act(lax.rem(me + k, n))
            return carry

        lax.fori_loop(1, n, step, 0)

    local_x = pltpu.make_async_copy(hidden_hbm, xg.at[me], x_local)
    local_g = pltpu.make_async_copy(gain_hbm, gg.at[me], g_local)
    local_x.start()
    local_g.start()

    barrier = pltpu.get_barrier_semaphore()
    each_peer(
        lambda peer: pl.semaphore_signal(
            barrier, inc=1, device_id={"tp": peer}, device_id_type=pl.DeviceIdType.MESH
        )
    )

    def start_wq(c, carry):
        wq_copy(c).start()
        return carry

    lax.fori_loop(0, n, start_wq, 0)
    copy_k = pltpu.make_async_copy(key_hbm, kv, kv_sem.at[0])
    copy_v = pltpu.make_async_copy(value_hbm, vv, kv_sem.at[1])
    copy_k.start()
    copy_v.start()

    def start_wo(k, carry):
        wo_copy(lax.rem(me + 1 + k, n)).start()
        return carry

    lax.fori_loop(0, n, start_wo, 0)

    local_x.wait()
    local_g.wait()
    pl.semaphore_wait(barrier, n - 1)

    def send_x(peer):
        remote(xg.at[me], xg.at[me], x_send.at[peer], x_recv.at[me], peer).start()
        remote(gg.at[me], gg.at[me], g_send.at[peer], g_recv.at[me], peer).start()

    each_peer(send_x)

    row4 = lax.broadcasted_iota(jnp.int32, (8, LANES), 0) % batch
    place = jnp.zeros((8, LANES), f32)
    for b in range(batch):
        place = jnp.where(row4 == b, pos_ref[b].astype(f32), place)
    angle = place * freq_ref[...]
    cosine = jnp.cos(angle)
    sine = jnp.sin(angle)
    lane8 = lax.broadcasted_iota(jnp.int32, (8, LANES), 1)
    sine = jnp.where(lane8 < HEAD_SIZE // 2, -sine, sine)

    def gain_piece(s, squares, peak):
        for j in range(dx // LANES):
            x = xg[s, :, j * LANES : (j + 1) * LANES].astype(f32)
            g = gg[s, j : j + 1, :].astype(f32)
            squares = squares + x * x
            y = x * g
            gained[s, :, j * LANES : (j + 1) * LANES] = y
            peak = jnp.maximum(peak, jnp.abs(y))
        return squares, peak

    zero = jnp.zeros((batch, LANES), f32)
    squares, peak = gain_piece(me, zero, zero)

    def take_x(k, carry):
        s = lax.rem(me + k, n)
        remote(xg.at[s], xg.at[s], x_send.at[s], x_recv.at[s], s).wait_recv()
        remote(gg.at[s], gg.at[s], g_send.at[s], g_recv.at[s], s).wait_recv()
        return gain_piece(s, *carry)

    squares, peak = lax.fori_loop(1, n, take_x, (squares, peak))
    rstd = lax.rsqrt(jnp.sum(squares, axis=-1, keepdims=True) / width + 1e-05)
    token_scale = (jnp.max(peak, axis=-1, keepdims=True) * rstd + 1e-06) / 448.0
    for b in range(batch):
        scale_ref[b] = jnp.max(token_scale[b : b + 1, :])

    per = 4 if n % 4 == 0 else 1

    def project(i, acc):
        for u in range(per):
            c = i * per + u
            wq_copy(c).wait()
            span = pl.ds(pl.multiple_of(c * dx, dx), dx)
            quant[:, span] = (gained[c] * rstd / token_scale).astype(bf16)
        span = pl.ds(pl.multiple_of(i * per * dx, per * dx), per * dx)
        return acc + lax.dot_general(
            wq[:, span], quant[:, span], (((1,), (1,)), ((), ())), preferred_element_type=f32
        )

    acc = lax.fori_loop(0, n // per, project, jnp.zeros((cw, batch), f32))
    proj = (acc.T * token_scale).astype(bf16).astype(f32)
    if padded > cw:
        proj = jnp.concatenate([proj, jnp.zeros((batch, padded - cw), f32)], axis=1)
    if cw % LANES:
        proj = pltpu.roll(proj, lax.rem(me * cw, LANES), 1)
    qg[me] = proj.astype(bf16)
    each_peer(
        lambda peer: remote(
            qg.at[me], qg.at[me], q_send.at[peer], q_recv.at[me], peer
        ).start()
    )
    each_peer(lambda s: remote(qg.at[s], qg.at[s], q_send.at[s], q_recv.at[s], s).wait_recv())

    total_heads = QUERY_HEADS + 2 * KEY_VALUE_HEADS
    for h in range(total_heads):
        piece = None
        for d in range(h * LANES // cw, (h * LANES + LANES - 1) // cw + 1):
            block = h - d * cw // LANES
            part = qg[d, :, block * LANES : (block + 1) * LANES].astype(f32)
            piece = part if piece is None else piece + part
        heads[h * batch : (h + 1) * batch, :] = piece

    def rotated(rows):
        count = rows.shape[0]
        turned = pltpu.roll(rows, HEAD_SIZE // 2, 1)
        return rows * jnp.tile(cosine, (count // 8, 1)) + turned * jnp.tile(sine, (count // 8, 1))

    copy_k.wait()
    copy_v.wait()
    inv = 1.0 / HEAD_SIZE**0.5
    rows_g = group * batch
    cols = batch * positions
    col = lax.broadcasted_iota(jnp.int32, (8, cols), 1)
    row = lax.broadcasted_iota(jnp.int32, (8, cols), 0)
    limit = jnp.zeros((8, cols), jnp.int32)
    for b in range(batch):
        limit = jnp.where(col // positions == b, lens_ref[b], limit)
    valid8 = (row % batch == col // positions) & (me * positions + col % positions < limit)
    bias8 = jnp.where(valid8, 0.0, -1e30)
    bias = jnp.tile(bias8, (rows_g // 8, 1))
    valid = bias == 0.0
    fresh_rows = rotated(
        heads[QUERY_HEADS * batch : (QUERY_HEADS + KEY_VALUE_HEADS) * batch, :]
    )
    lane = lax.broadcasted_iota(jnp.int32, (rows_g, LANES), 1)
    for g in range(KEY_VALUE_HEADS):
        q = rotated(heads[g * rows_g : (g + 1) * rows_g, :]).astype(bf16)
        k_rows = kv[:, :, g * HEAD_SIZE : (g + 1) * HEAD_SIZE].reshape(cols, HEAD_SIZE)
        v_rows = vv[:, :, g * HEAD_SIZE : (g + 1) * HEAD_SIZE].reshape(cols, HEAD_SIZE)
        s = (
            lax.dot_general(q, k_rows, (((1,), (1,)), ((), ())), preferred_element_type=f32) * inv
        )
        top = jnp.max(jnp.where(valid, s, -1e30), axis=-1, keepdims=True)
        w = jnp.where(valid, jnp.exp(s - top), 0.0)
        total = jnp.sum(w, axis=-1, keepdims=True)
        o = jnp.dot(w.astype(bf16), v_rows, preferred_element_type=f32)
        k_new = fresh_rows[g * batch : (g + 1) * batch, :]
        base = (QUERY_HEADS + KEY_VALUE_HEADS + g) * batch
        v_new = heads[base : base + batch, :]
        s_new = (
            jnp.sum(q.astype(f32) * jnp.tile(k_new, (group, 1)), axis=-1, keepdims=True) * inv
        )
        s_new = jnp.where(me == 0, s_new, -1e30)
        top_new = jnp.maximum(top, s_new)
        keep = jnp.exp(top - top_new)
        fresh = jnp.where(me == 0, jnp.exp(s_new - top_new), 0.0)
        total = total * keep + fresh
        o = o * keep + fresh * jnp.tile(v_new, (group, 1))
        some = total > 0.0
        safe = jnp.where(some, total, 1.0)
        o = o / safe
        lse = jnp.where(some, top_new + jnp.log(safe), -1e30)
        hi = lse.astype(bf16).astype(f32)
        rest = lse - hi
        mid = rest.astype(bf16).astype(f32)
        low = rest - mid
        tail = jnp.where(
            lane == 0, hi, jnp.where(lane == 1, mid, jnp.where(lane == 2, low, 0.0))
        )
        both = jnp.concatenate([o, tail], axis=1).astype(bf16)
        for j in range(group // own_heads):
            so[g * (group // own_heads) + j] = both[j * own_rows : (j + 1) * own_rows, :]

    each_peer(
        lambda peer: remote(
            so.at[peer], og.at[me], o_send.at[peer], o_recv.at[me], peer
        ).start()
    )
    og[me] = so[me]
    each_peer(lambda s: remote(so.at[s], og.at[s], o_send.at[s], o_recv.at[s], s).wait_recv())

    lses = [
        jnp.sum(og[s, :, LANES : 2 * LANES].astype(f32), axis=-1, keepdims=True) for s in range(n)
    ]
    best = functools.reduce(jnp.maximum, lses)
    den = jnp.zeros_like(best)
    num = jnp.zeros((own_rows, LANES), f32)
    for s in range(n):
        share = jnp.exp(lses[s] - best)
        den = den + share
        num = num + share * og[s, :, 0:LANES].astype(f32)
    att = num / den
    att = jnp.concatenate(
        [att[j * batch : (j + 1) * batch, :] for j in range(own_heads)], axis=1
    ).astype(bf16)

    def project_out(k, carry):
        e = lax.rem(me + 1 + k, n)
        wo_copy(e).wait()
        rs_send[e] = jnp.dot(att, wo[e], preferred_element_type=f32).astype(bf16)
        remote(rs_send.at[e], rs_recv.at[me], r_send.at[e], r_recv.at[me], e).start()
        return carry

    lax.fori_loop(0, n - 1, project_out, 0)
    wo_copy(me).wait()
    own = jnp.dot(att, wo[me], preferred_element_type=f32)

    def take_r(k, carry):
        s = lax.rem(me + k, n)
        remote(rs_send.at[s], rs_recv.at[s], r_send.at[s], r_recv.at[s], s).wait_recv()
        return carry + rs_recv[s].astype(f32)

    out_ref[...] = lax.fori_loop(1, n, take_r, own).astype(bf16)

    def finish(peer):
        remote(xg.at[me], xg.at[me], x_send.at[peer], x_recv.at[me], peer).wait_send()
        remote(gg.at[me], gg.at[me], g_send.at[peer], g_recv.at[me], peer).wait_send()
        remote(qg.at[me], qg.at[me], q_send.at[peer], q_recv.at[me], peer).wait_send()
        remote(so.at[peer], og.at[me], o_send.at[peer], o_recv.at[me], peer).wait_send()
        remote(rs_send.at[peer], rs_recv.at[me], r_send.at[peer], r_recv.at[me], peer).wait_send()

    each_peer(finish)


def on_device(n, hidden_in, norm_gain, w_qkv, w_out, key_cache, value_cache, lengths, positions):
    batch, dx = hidden_in.shape
    cw = w_qkv.shape[1]
    own_rows = w_out.shape[0] // HEAD_SIZE * batch
    total_heads = QUERY_HEADS + 2 * KEY_VALUE_HEADS
    widest = max(d * cw % LANES for d in range(n)) + cw
    padded = rounded_up(widest, LANES)
    half = HEAD_SIZE // 2
    freq = np.float32(500000.0) ** (
        -(np.arange(half, dtype=np.float32) * np.float32(2.0)) / np.float32(HEAD_SIZE)
    )
    freq = jnp.asarray(np.tile(freq.astype(np.float32), 2)[None, :])
    bf16, f32 = jnp.bfloat16, jnp.float32
    dma = pltpu.SemaphoreType.DMA
    hbm = pl.BlockSpec(memory_space=pl.ANY)
    smem = pl.BlockSpec(memory_space=pltpu.SMEM)
    vmem = pl.BlockSpec(memory_space=pltpu.VMEM)
    return pl.pallas_call(
        functools.partial(kernel, n),
        out_shape=(
            jax.ShapeDtypeStruct((batch, dx), bf16),
            jax.ShapeDtypeStruct((batch,), f32),
        ),
        in_specs=[hbm] * 6 + [smem, smem, vmem],
        out_specs=(vmem, smem),
        scratch_shapes=[
            pltpu.VMEM((n, batch, dx), bf16),
            pltpu.VMEM((n, dx // LANES, LANES), bf16),
            pltpu.VMEM((n, batch, dx), f32),
            pltpu.VMEM((batch, n * dx), bf16),
            pltpu.VMEM((cw, n * dx), bf16),
            pltpu.VMEM((n, w_out.shape[0], dx), bf16),
            pltpu.VMEM(key_cache.shape, bf16),
            pltpu.VMEM(value_cache.shape, bf16),
            pltpu.VMEM((n, batch, padded), bf16),
            pltpu.VMEM((total_heads * batch, HEAD_SIZE), f32),
            pltpu.VMEM((n, own_rows, 2 * LANES), bf16),
            pltpu.VMEM((n, own_rows, 2 * LANES), bf16),
            pltpu.VMEM((n, batch, dx), bf16),
            pltpu.VMEM((n, batch, dx), bf16),
            dma(()),
            dma(()),
            dma((n,)),
            dma((n,)),
            dma((2,)),
        ]
        + [dma((n,))] * 10,
        compiler_params=pltpu.CompilerParams(
            collective_id=0, has_side_effects=True, vmem_limit_bytes=60 * 1024 * 1024
        ),
        name="decode",
    )(
        hidden_in,
        norm_gain.reshape(dx // LANES, LANES),
        w_qkv.T,
        w_out,
        key_cache,
        value_cache,
        lengths,
        positions,
        freq,
    )


def solution(mesh):
    placed = (
        P("replica", "tp"),
        P("tp"),
        P(None, "tp"),
        P("tp", None),
        P("replica", "tp", None),
        P("replica", "tp", None),
        P("replica"),
        P("replica"),
    )
    return jax.shard_map(
        functools.partial(on_device, mesh.shape["tp"]),
        mesh=mesh,
        in_specs=placed,
        out_specs=(P("replica", "tp"), P("replica")),
        check_vma=False,
    )
```

```python
import functools

import jax
import jax.numpy as jnp
import numpy as np
from jax import lax
from jax.experimental import pallas as pl
from jax.experimental.pallas import tpu as pltpu
from jax.sharding import PartitionSpec as P

QUERY_HEADS = 64
KEY_VALUE_HEADS = 4
HEAD_SIZE = 128
LANES = 128


def rounded_up(value, step):
    return (value + step - 1) // step * step


def kernel(
    n,
    hidden_hbm,
    gain_hbm,
    wq_hbm,
    wo_hbm,
    key_hbm,
    value_hbm,
    lens_ref,
    pos_ref,
    freq_ref,
    out_ref,
    scale_ref,
    xg,
    gained,
    quant,
    wq,
    wo,
    kv,
    vv,
    stage,
    qg,
    heads,
    so,
    og,
    rs_send,
    rs_recv,
    x_local,
    g_local,
    wq_sem,
    wo_sem,
    kv_sem,
    x_send,
    x_recv,
    q_send,
    q_recv,
    o_send,
    o_recv,
    r_send,
    r_recv,
):
    me = lax.axis_index("tp")
    dx = wo.shape[2]
    batch = lens_ref.shape[0]
    pieces = dx // LANES
    x_rows = pieces * batch
    gain_at = xg.shape[1] - rounded_up(pieces, 8)
    cw, width = wq_hbm.shape
    blocks = stage.shape[0] // batch
    padded = blocks * LANES
    own_rows = og.shape[1]
    own_heads = own_rows // batch
    positions = key_hbm.shape[1]
    group = QUERY_HEADS // KEY_VALUE_HEADS
    f32, bf16 = jnp.float32, jnp.bfloat16

    def wq_copy(c):
        span = pl.ds(pl.multiple_of(c * dx, dx), dx)
        return pltpu.make_async_copy(wq_hbm.at[:, span], wq.at[:, span], wq_sem.at[c])

    def wo_copy(c):
        return pltpu.make_async_copy(
            wo_hbm.at[:, pl.ds(pl.multiple_of(c * dx, dx), dx)], wo.at[c], wo_sem.at[c]
        )

    def remote(src, dst, send, recv, peer):
        return pltpu.make_async_remote_copy(
            src_ref=src,
            dst_ref=dst,
            send_sem=send,
            recv_sem=recv,
            device_id={"tp": peer},
            device_id_type=pl.DeviceIdType.MESH,
        )

    def each_peer(act):
        def step(k, carry):
            act(lax.rem(me + k, n))
            return carry

        lax.fori_loop(1, n, step, 0)

    local_x = pltpu.make_async_copy(hidden_hbm, xg.at[me, pl.ds(0, x_rows), :], x_local)
    local_g = pltpu.make_async_copy(gain_hbm, xg.at[me, pl.ds(gain_at, pieces), :], g_local)
    local_x.start()
    local_g.start()

    barrier = pltpu.get_barrier_semaphore()
    each_peer(
        lambda peer: pl.semaphore_signal(
            barrier, inc=1, device_id={"tp": peer}, device_id_type=pl.DeviceIdType.MESH
        )
    )

    def start_wq(c, carry):
        wq_copy(c).start()
        return carry

    lax.fori_loop(0, n, start_wq, 0)
    copy_k = pltpu.make_async_copy(key_hbm, kv, kv_sem.at[0])
    copy_v = pltpu.make_async_copy(value_hbm, vv, kv_sem.at[1])
    copy_k.start()
    copy_v.start()

    def start_wo(k, carry):
        wo_copy(lax.rem(me + 1 + k, n)).start()
        return carry

    lax.fori_loop(0, n, start_wo, 0)

    local_x.wait()
    local_g.wait()
    pl.semaphore_wait(barrier, n - 1)

    def send_x(peer):
        remote(xg.at[me], xg.at[me], x_send.at[peer], x_recv.at[me], peer).start()

    each_peer(send_x)

    row4 = lax.broadcasted_iota(jnp.int32, (8, LANES), 0) % batch
    place = jnp.zeros((8, LANES), f32)
    for b in range(batch):
        place = jnp.where(row4 == b, pos_ref[b].astype(f32), place)
    angle = place * freq_ref[...]
    cosine = jnp.cos(angle)
    sine = jnp.sin(angle)
    lane8 = lax.broadcasted_iota(jnp.int32, (8, LANES), 1)
    sine = jnp.where(lane8 < HEAD_SIZE // 2, -sine, sine)

    half8 = lax.broadcasted_iota(jnp.int32, (8, LANES), 0) // batch
    per8 = 8 // batch

    def gain_piece(s, squares, peak):
        x = xg[s, 0:x_rows, :].astype(f32)
        g = xg[s, gain_at : gain_at + rounded_up(pieces, 8), :].astype(f32)
        for j in range(x_rows // 8):
            x8 = x[8 * j : 8 * j + 8, :]
            g8 = jnp.zeros((8, LANES), f32)
            for u in range(per8):
                r = j * per8 + u
                g8 = jnp.where(half8 == u, g[r : r + 1, :], g8)
            squares = squares + x8 * x8
            y = x8 * g8
            gained[s, 8 * j : 8 * j + 8, :] = y
            peak = jnp.maximum(peak, jnp.abs(y))
        return squares, peak

    zero = jnp.zeros((8, LANES), f32)
    squares, peak = gain_piece(me, zero, zero)

    def take_x(k, carry):
        s = lax.rem(me + k, n)
        remote(xg.at[s], xg.at[s], x_send.at[s], x_recv.at[s], s).wait_recv()
        return gain_piece(s, *carry)

    squares, peak = lax.fori_loop(1, n, take_x, (squares, peak))
    squares = sum(squares[u * batch : (u + 1) * batch, :] for u in range(per8))
    peak = functools.reduce(
        jnp.maximum, [peak[u * batch : (u + 1) * batch, :] for u in range(per8)]
    )
    rstd = lax.rsqrt(jnp.sum(squares, axis=-1, keepdims=True) / width + 1e-05)
    token_scale = (jnp.max(peak, axis=-1, keepdims=True) * rstd + 1e-06) / 448.0
    rstd_rows = jnp.tile(jnp.broadcast_to(rstd, (batch, LANES)), (per8, 1))
    scale_rows = jnp.tile(jnp.broadcast_to(token_scale, (batch, LANES)), (per8, 1))
    rstd_rows = jnp.tile(rstd_rows, (x_rows // 8, 1))
    scale_rows = jnp.tile(scale_rows, (x_rows // 8, 1))
    for b in range(batch):
        scale_ref[b] = jnp.max(token_scale[b : b + 1, :])

    per = 4 if n % 4 == 0 else 1

    def project(i, acc):
        for u in range(per):
            c = i * per + u
            wq_copy(c).wait()
            span = pl.ds(pl.multiple_of(c * dx, dx), dx)
            rows = gained[c] * rstd_rows / scale_rows
            quant[:, span] = jnp.concatenate(
                [rows[j * batch : (j + 1) * batch, :] for j in range(pieces)], axis=1
            ).astype(bf16)
        span = pl.ds(pl.multiple_of(i * per * dx, per * dx), per * dx)
        return acc + lax.dot_general(
            wq[:, span], quant[:, span], (((1,), (1,)), ((), ())), preferred_element_type=f32
        )

    acc = lax.fori_loop(0, n // per, project, jnp.zeros((cw, batch), f32))
    proj = (acc.T * token_scale).astype(bf16).astype(f32)
    if padded > cw:
        proj = jnp.concatenate([proj, jnp.zeros((batch, padded - cw), f32)], axis=1)
    if cw % LANES:
        proj = pltpu.roll(proj, lax.rem(me * cw, LANES), 1)
    for j in range(blocks):
        stage[j * batch : (j + 1) * batch, :] = proj[:, j * LANES : (j + 1) * LANES]
    qg[me, 0 : blocks * batch, :] = stage[...].astype(bf16)
    each_peer(
        lambda peer: remote(
            qg.at[me], qg.at[me], q_send.at[peer], q_recv.at[me], peer
        ).start()
    )
    each_peer(lambda s: remote(qg.at[s], qg.at[s], q_send.at[s], q_recv.at[s], s).wait_recv())

    total_heads = QUERY_HEADS + 2 * KEY_VALUE_HEADS
    unpacked = [qg[d].astype(f32) for d in range(n)]
    for h in range(total_heads):
        piece = None
        for d in range(h * LANES // cw, (h * LANES + LANES - 1) // cw + 1):
            block = h - d * cw // LANES
            part = unpacked[d][block * batch : (block + 1) * batch, :]
            piece = part if piece is None else piece + part
        heads[h * batch : (h + 1) * batch, :] = piece

    def rotated(rows):
        count = rows.shape[0]
        turned = pltpu.roll(rows, HEAD_SIZE // 2, 1)
        return rows * jnp.tile(cosine, (count // 8, 1)) + turned * jnp.tile(sine, (count // 8, 1))

    copy_k.wait()
    copy_v.wait()
    inv = 1.0 / HEAD_SIZE**0.5
    rows_g = group * batch
    cols = batch * positions
    col = lax.broadcasted_iota(jnp.int32, (8, cols), 1)
    row = lax.broadcasted_iota(jnp.int32, (8, cols), 0)
    limit = jnp.zeros((8, cols), jnp.int32)
    for b in range(batch):
        limit = jnp.where(col // positions == b, lens_ref[b], limit)
    valid8 = (row % batch == col // positions) & (me * positions + col % positions < limit)
    bias8 = jnp.where(valid8, 0.0, -1e30)
    bias = jnp.tile(bias8, (rows_g // 8, 1))
    valid = bias == 0.0
    fresh_rows = rotated(
        heads[QUERY_HEADS * batch : (QUERY_HEADS + KEY_VALUE_HEADS) * batch, :]
    )
    lane = lax.broadcasted_iota(jnp.int32, (rows_g, LANES), 1)
    for g in range(KEY_VALUE_HEADS):
        q = rotated(heads[g * rows_g : (g + 1) * rows_g, :]).astype(bf16)
        k_rows = kv[:, :, g * HEAD_SIZE : (g + 1) * HEAD_SIZE].reshape(cols, HEAD_SIZE)
        v_rows = vv[:, :, g * HEAD_SIZE : (g + 1) * HEAD_SIZE].reshape(cols, HEAD_SIZE)
        s = (
            lax.dot_general(q, k_rows, (((1,), (1,)), ((), ())), preferred_element_type=f32) * inv
        )
        top = jnp.max(jnp.where(valid, s, -1e30), axis=-1, keepdims=True)
        w = jnp.where(valid, jnp.exp(s - top), 0.0)
        total = jnp.sum(w, axis=-1, keepdims=True)
        o = jnp.dot(w.astype(bf16), v_rows, preferred_element_type=f32)
        k_new = fresh_rows[g * batch : (g + 1) * batch, :]
        base = (QUERY_HEADS + KEY_VALUE_HEADS + g) * batch
        v_new = heads[base : base + batch, :]
        s_new = (
            jnp.sum(q.astype(f32) * jnp.tile(k_new, (group, 1)), axis=-1, keepdims=True) * inv
        )
        s_new = jnp.where(me == 0, s_new, -1e30)
        top_new = jnp.maximum(top, s_new)
        keep = jnp.exp(top - top_new)
        fresh = jnp.where(me == 0, jnp.exp(s_new - top_new), 0.0)
        total = total * keep + fresh
        o = o * keep + fresh * jnp.tile(v_new, (group, 1))
        some = total > 0.0
        safe = jnp.where(some, total, 1.0)
        o = o / safe
        lse = jnp.where(some, top_new + jnp.log(safe), -1e30)
        hi = lse.astype(bf16).astype(f32)
        rest = lse - hi
        mid = rest.astype(bf16).astype(f32)
        low = rest - mid
        tail = jnp.where(
            lane == 0, hi, jnp.where(lane == 1, mid, jnp.where(lane == 2, low, 0.0))
        )
        both = jnp.concatenate([o, tail], axis=1).astype(bf16)
        for j in range(group // own_heads):
            so[g * (group // own_heads) + j] = both[j * own_rows : (j + 1) * own_rows, :]

    each_peer(
        lambda peer: remote(
            so.at[peer], og.at[me], o_send.at[peer], o_recv.at[me], peer
        ).start()
    )
    og[me] = so[me]
    each_peer(lambda s: remote(so.at[s], og.at[s], o_send.at[s], o_recv.at[s], s).wait_recv())

    lses = [
        jnp.sum(og[s, :, LANES : 2 * LANES].astype(f32), axis=-1, keepdims=True) for s in range(n)
    ]
    best = functools.reduce(jnp.maximum, lses)
    den = jnp.zeros_like(best)
    num = jnp.zeros((own_rows, LANES), f32)
    for s in range(n):
        share = jnp.exp(lses[s] - best)
        den = den + share
        num = num + share * og[s, :, 0:LANES].astype(f32)
    att = num / den
    att = jnp.concatenate(
        [att[j * batch : (j + 1) * batch, :] for j in range(own_heads)], axis=1
    ).astype(bf16)

    def rows_of(part):
        return jnp.concatenate(
            [part[:, j * LANES : (j + 1) * LANES] for j in range(pieces)], axis=0
        )

    unroll = 3 if (n - 1) % 3 == 0 else 1

    def project_out(i, carry):
        parts = []
        for u in range(unroll):
            e = lax.rem(me + 1 + i * unroll + u, n)
            wo_copy(e).wait()
            parts.append(jnp.dot(att, wo[e], preferred_element_type=f32))
        for u in range(unroll):
            e = lax.rem(me + 1 + i * unroll + u, n)
            rs_send[e] = rows_of(parts[u]).astype(bf16)
            remote(rs_send.at[e], rs_recv.at[me], r_send.at[e], r_recv.at[me], e).start()
        return carry

    lax.fori_loop(0, (n - 1) // unroll, project_out, 0)
    wo_copy(me).wait()
    own = rows_of(jnp.dot(att, wo[me], preferred_element_type=f32))

    def take_r(k, carry):
        s = lax.rem(me + k, n)
        remote(rs_send.at[s], rs_recv.at[s], r_send.at[s], r_recv.at[s], s).wait_recv()
        return carry + rs_recv[s].astype(f32)

    out_ref[...] = lax.fori_loop(1, n, take_r, own).astype(bf16)

    def finish(peer):
        remote(xg.at[me], xg.at[me], x_send.at[peer], x_recv.at[me], peer).wait_send()
        remote(qg.at[me], qg.at[me], q_send.at[peer], q_recv.at[me], peer).wait_send()
        remote(so.at[peer], og.at[me], o_send.at[peer], o_recv.at[me], peer).wait_send()
        remote(rs_send.at[peer], rs_recv.at[me], r_send.at[peer], r_recv.at[me], peer).wait_send()

    each_peer(finish)


def on_device(n, hidden_in, norm_gain, w_qkv, w_out, key_cache, value_cache, lengths, positions):
    batch, dx = hidden_in.shape
    cw = w_qkv.shape[1]
    own_rows = w_out.shape[0] // HEAD_SIZE * batch
    total_heads = QUERY_HEADS + 2 * KEY_VALUE_HEADS
    widest = max(d * cw % LANES for d in range(n)) + cw
    blocks = rounded_up(widest, LANES) // LANES
    pieces = dx // LANES
    x_height = rounded_up(pieces * batch, 8) + rounded_up(pieces, 8)
    half = HEAD_SIZE // 2
    freq = np.float32(500000.0) ** (
        -(np.arange(half, dtype=np.float32) * np.float32(2.0)) / np.float32(HEAD_SIZE)
    )
    freq = jnp.asarray(np.tile(freq.astype(np.float32), 2)[None, :])
    bf16, f32 = jnp.bfloat16, jnp.float32
    dma = pltpu.SemaphoreType.DMA
    hbm = pl.BlockSpec(memory_space=pl.ANY)
    smem = pl.BlockSpec(memory_space=pltpu.SMEM)
    vmem = pl.BlockSpec(memory_space=pltpu.VMEM)
    out, token_scale = pl.pallas_call(
        functools.partial(kernel, n),
        out_shape=(
            jax.ShapeDtypeStruct((pieces * batch, LANES), bf16),
            jax.ShapeDtypeStruct((batch,), f32),
        ),
        in_specs=[hbm] * 6 + [smem, smem, vmem],
        out_specs=(vmem, smem),
        scratch_shapes=[
            pltpu.VMEM((n, x_height, LANES), bf16),
            pltpu.VMEM((n, pieces * batch, LANES), f32),
            pltpu.VMEM((batch, n * dx), bf16),
            pltpu.VMEM((cw, n * dx), bf16),
            pltpu.VMEM((n, w_out.shape[0], dx), bf16),
            pltpu.VMEM(key_cache.shape, bf16),
            pltpu.VMEM(value_cache.shape, bf16),
            pltpu.VMEM((blocks * batch, LANES), f32),
            pltpu.VMEM((n, rounded_up(blocks * batch, 8), LANES), bf16),
            pltpu.VMEM((total_heads * batch, HEAD_SIZE), f32),
            pltpu.VMEM((n, own_rows, 2 * LANES), bf16),
            pltpu.VMEM((n, own_rows, 2 * LANES), bf16),
            pltpu.VMEM((n, pieces * batch, LANES), bf16),
            pltpu.VMEM((n, pieces * batch, LANES), bf16),
            dma(()),
            dma(()),
            dma((n,)),
            dma((n,)),
            dma((2,)),
        ]
        + [dma((n,))] * 8,
        compiler_params=pltpu.CompilerParams(
            collective_id=0, has_side_effects=True, vmem_limit_bytes=60 * 1024 * 1024
        ),
        name="decode",
    )(
        hidden_in.reshape(batch, pieces, LANES).transpose(1, 0, 2).reshape(-1, LANES),
        norm_gain.reshape(dx // LANES, LANES),
        w_qkv.T,
        w_out,
        key_cache,
        value_cache,
        lengths,
        positions,
        freq,
    )
    out = out.reshape(pieces, batch, LANES).transpose(1, 0, 2).reshape(batch, dx)
    return out, token_scale


def solution(mesh):
    placed = (
        P("replica", "tp"),
        P("tp"),
        P(None, "tp"),
        P("tp", None),
        P("replica", "tp", None),
        P("replica", "tp", None),
        P("replica"),
        P("replica"),
    )
    return jax.shard_map(
        functools.partial(on_device, mesh.shape["tp"]),
        mesh=mesh,
        in_specs=placed,
        out_specs=(P("replica", "tp"), P("replica")),
        check_vma=False,
    )
```
